128 devices in a mesh: grp: 4 (over z), leaf: 32 (over y, x, core).
Axes of the slice: x: 4, y: 4, z: 4, core: 2. Of those that a mesh axis runs over, the one named last changes fastest.
Arguments:
- basis_slab: bfloat16 [131072, 1024], P(('grp', 'leaf')), may hold values from -6 to 6
- live_counts: int32 [128], P(('grp', 'leaf')), may hold values from 128 to 1024, as said below
- pole_order: int32 [128, 1024], P(('grp', 'leaf')), may hold values from 0 to 1023, each once within a row
- leaf_diag: bfloat16 [131072, 1024], P(('grp', 'leaf')), may hold values from -0.1875 to 0.1875
- leaf_in: bfloat16 [131072, 128], P(('grp', 'leaf')), may hold values from -0.1875 to 0.1875
- leaf_out: bfloat16 [131072, 128], P(('grp', 'leaf')), may hold values from -0.5 to 0.5
- leaf_lift: bfloat16 [128, 128, 128], P(('grp', 'leaf')), may hold values from -0.375 to 0.375
- leaf_couple: bfloat16 [128, 128, 128], P(('grp', 'leaf')), may hold values from -0.5 to 0.5
- leaf_spread: bfloat16 [128, 128, 128], P(('grp', 'leaf')), may hold values from -0.4375 to 0.4375
- inner_lift: bfloat16 [124, 128, 128], replicated, may hold values from -0.375 to 0.375
- inner_couple: bfloat16 [126, 128, 128], replicated, may hold values from -0.5 to 0.5
- inner_spread: bfloat16 [124, 128, 128], replicated, may hold values from -0.4375 to 0.4375
Outputs:
- merged: bfloat16 [131072, 1024], P(('grp', 'leaf'))
The draws below stay inside these ranges and needn't reach their ends.
Inputs may be any that keep to these rules, and one draw needn't show every extreme that they name: `live_counts`: each count is 1024, 512, 256 or 128, and some leaf has 1024. `pole_order`: each row names every slot's pole once.
All inputs are finite; a program needn't handle non-finite values.
Results may differ from the reference program's by a relative error of at most 0.0055.
Values may be sent and summed in bfloat16 or wider, within the bound.
No kernel may reach another device: no remote copies, remote signals or barrier semaphores. Data moves between devices by JAX's collectives and lax.ppermute only.
A program may use at most 64 MiB of HBM per device.

```python
import jax
import jax.numpy as jnp
from jax import lax

M = 1024
RANK = 128
R = 1024
N = 131072
N_GRP = 4
N_LEAF = 32
DEVICES = 128


def draw_live_counts(key, part):
    first_key, second_key = jax.random.split(jax.random.fold_in(key, 17))
    halvings = jax.random.randint(first_key, (N_GRP * N_LEAF,), 0, 4)
    counts = jnp.right_shift(jnp.full((N_GRP * N_LEAF,), M, jnp.int32), halvings.astype(jnp.int32))
    fullest = jax.random.randint(second_key, (), 0, N_GRP * N_LEAF)
    return counts.at[fullest].set(M).astype(jnp.int32)


def block_scale(key, dims, cuts, low, largest):
    gain = 1.0
    for axis_at, parts in cuts:
        draws = jax.random.uniform(jax.random.fold_in(jax.random.fold_in(key, 6), axis_at), (parts,), jnp.float32, low / len(cuts), largest / len(cuts))
        gain = gain * jnp.repeat(jnp.exp(draws), dims[axis_at] // parts).reshape((-1,) + (1,) * (len(dims) - 1 - axis_at))
    return gain


def scatter_about(key, extent, spread, limit, cuts=(), kind=jnp.bfloat16):
    drawn = spread * jax.random.normal(key, extent, jnp.float32)
    if cuts:
        drawn = drawn * block_scale(key, extent, cuts, -0.22, 0.18)
    return jnp.clip(drawn, -limit, limit).astype(kind)


def setup_inputs(seed: int = 0) -> dict:
    seeds = jax.random.split(jax.random.key(seed), 13)
    return {
        "basis_slab": scatter_about(seeds[0], (N, R), 1.0, 6.0, ((0, 128),)),
        "live_counts": draw_live_counts(jax.random.fold_in(seeds[12], 71), 0),
        "pole_order": jax.vmap(lambda own: jax.random.permutation(own, M))(jax.random.split(seeds[2], DEVICES)).reshape((DEVICES, M)).astype(jnp.int32),
        "leaf_diag": scatter_about(seeds[3], (N, M), M ** -0.5, 0.1875, ((0, 128),)),
        "leaf_in": scatter_about(seeds[4], (N, RANK), M ** -0.5, 0.1875, ((0, 128),)),
        "leaf_out": scatter_about(seeds[5], (N, RANK), RANK ** -0.5, 0.5, ((0, 128),)),
        "leaf_lift": scatter_about(seeds[6], (DEVICES, RANK, RANK), (2 * RANK) ** -0.5, 0.375, ((0, 128),)),
        "leaf_couple": scatter_about(seeds[7], (DEVICES, RANK, RANK), RANK ** -0.5, 0.5, ((0, 128),)),
        "leaf_spread": scatter_about(seeds[8], (DEVICES, RANK, RANK), (3 * RANK // 2) ** -0.5, 0.4375, ((0, 128),)),
        "inner_lift": scatter_about(seeds[9], (DEVICES - 4, RANK, RANK), (2 * RANK) ** -0.5, 0.375),
        "inner_couple": scatter_about(seeds[10], (DEVICES - 2, RANK, RANK), RANK ** -0.5, 0.5),
        "inner_spread": scatter_about(seeds[11], (DEVICES - 4, RANK, RANK), (3 * RANK // 2) ** -0.5, 0.4375),
    }


def full_product(matrices, stacked):
    return jnp.einsum('nij,njc->nic', matrices.astype(jnp.float32), stacked, precision=lax.Precision.HIGHEST)


def leaf_skeleton(pieces):
    generator, masked = pieces
    return jnp.einsum('mk,mc->kc', generator, masked, preferred_element_type=jnp.float32)


def leaf_update(pieces):
    diagonal, generator, masked, incoming = pieces
    return jnp.dot(diagonal, masked, preferred_element_type=jnp.float32) + jnp.dot(generator, incoming, preferred_element_type=jnp.float32)


def reference(basis_slab, live_counts, pole_order, leaf_diag, leaf_in, leaf_out, leaf_lift, leaf_couple, leaf_spread, inner_lift, inner_couple, inner_spread):
    devices = N_GRP * N_LEAF
    block_rows = M // devices
    levels = devices.bit_length() - 1
    leaf_rows = basis_slab.reshape(devices, devices, block_rows, R).transpose(1, 0, 2, 3).reshape(devices, M, R)
    slots = jnp.take_along_axis(leaf_rows, pole_order.astype(jnp.int32)[:, :, None], axis=1)
    live_mask = jnp.arange(M, dtype=jnp.int32)[None, :] < live_counts[:, None]
    masked = jnp.where(live_mask[:, :, None], slots, jnp.zeros_like(slots))
    skeleton = lax.map(leaf_skeleton, (leaf_in.reshape(devices, M, RANK), masked))
    crosses = []
    for height in range(levels):
        node_count = devices >> height
        couples = leaf_couple if height == 0 else inner_couple[node_count - 2:2 * node_count - 2]
        coupled = full_product(couples, skeleton)
        crosses.append(coupled.reshape(node_count // 2, 2, RANK, R)[:, ::-1].reshape(node_count, RANK, R))
        if height < levels - 1:
            lifts = leaf_lift if height == 0 else inner_lift[node_count - 4:2 * node_count - 4]
            lifted = full_product(lifts, skeleton)
            skeleton = lifted[0::2] + lifted[1::2]
    incoming = crosses[levels - 1]
    for height in range(levels - 2, -1, -1):
        node_count = devices >> height
        spreads = leaf_spread if height == 0 else inner_spread[node_count - 4:2 * node_count - 4]
        parent = jnp.repeat(incoming, 2, axis=0)
        incoming = full_product(spreads, parent) + crosses[height]
    incoming_b = incoming.astype(jnp.bfloat16)
    updated = lax.map(leaf_update, (leaf_diag.reshape(devices, M, M), leaf_out.reshape(devices, M, RANK), masked, incoming_b))
    updated = jnp.where(live_mask[:, :, None], updated, slots.astype(jnp.float32)).astype(jnp.bfloat16)
    inverse = jnp.zeros((devices, M), jnp.int32).at[jnp.arange(devices, dtype=jnp.int32)[:, None], pole_order.astype(jnp.int32)].set(jnp.broadcast_to(jnp.arange(M, dtype=jnp.int32), (devices, M)))
    restored = jnp.take_along_axis(updated, inverse[:, :, None], axis=1)
    return restored.reshape(devices, devices, block_rows, R).transpose(1, 0, 2, 3).reshape(N, R)
```

```python
import functools

import jax
import jax.numpy as jnp
from jax import lax
from jax.experimental import pallas as pl
from jax.experimental.pallas import tpu as pltpu
from jax.sharding import PartitionSpec as P

BOTH = ("grp", "leaf")
NT = (((1,), (1,)), ((), ()))
TN = (((0,), (0,)), ((), ()))


def exchange(blocks):
    return lax.all_to_all(blocks, BOTH, split_axis=0, concat_axis=0, tiled=True)


def dot(a, b, dims):
    return lax.dot_general(a, b, dims, preferred_element_type=jnp.float32)


def split_rows(value):
    head = value.astype(jnp.bfloat16).astype(jnp.float32)
    return jnp.concatenate([head, value - head], axis=0).astype(jnp.bfloat16)


def times_transposed(pair, matrix):
    both = dot(pair, matrix, NT)
    rows = both.shape[0] // 2
    return both[:rows] + both[rows:]


def tree_kernel(
    levels, parts_ref, lift_hbm, couple_hbm, spread_hbm, out_ref, lift, couple, spread, cross, sems
):
    copies = {}
    inner = levels - 1
    slot = 0

    def fetch(name, source, target, start, size):
        nonlocal slot
        copy = pltpu.make_async_copy(
            source.at[pl.ds(start, size)], target.at[pl.ds(start, size)], sems.at[slot]
        )
        copy.start()
        copies[name] = copy
        slot += 1

    for height in range(1, levels):
        nodes = 1 << (levels - height)
        if height < inner:
            fetch(("lift", height), lift_hbm, lift, nodes - 4, nodes)
        fetch(("couple", height), couple_hbm, couple, nodes - 2, nodes)
    for height in range(inner - 1, 0, -1):
        nodes = 1 << (levels - height)
        fetch(("spread", height), spread_hbm, spread, nodes - 4, nodes)

    count = 1 << inner
    skeletons = [
        parts_ref[2 * n].astype(jnp.float32) + parts_ref[2 * n + 1].astype(jnp.float32)
        for n in range(count)
    ]
    for height in range(1, levels):
        nodes = 1 << (levels - height)
        if height < inner:
            copies["lift", height].wait()
        copies["couple", height].wait()
        lifted = []
        for n in range(nodes):
            pair = split_rows(skeletons[n])
            cross[nodes - 2 + (n ^ 1)] = times_transposed(pair, couple[nodes - 2 + n])
            if height < inner:
                lifted.append(times_transposed(pair, lift[nodes - 4 + n]))
        skeletons = [lifted[n] + lifted[n + 1] for n in range(0, len(lifted), 2)]
    incoming = [cross[0], cross[1]]
    for height in range(inner - 1, 0, -1):
        nodes = 1 << (levels - height)
        copies["spread", height].wait()
        below = []
        for parent in range(nodes // 2):
            pair = split_rows(incoming[parent])
            for child in (2 * parent, 2 * parent + 1):
                below.append(
                    times_transposed(pair, spread[nodes - 4 + child]) + cross[nodes - 2 + child]
                )
        incoming = below
    for n in range(count):
        value = incoming[n].astype(out_ref.dtype)
        out_ref[2 * n] = value
        out_ref[2 * n + 1] = value


def tree(parts, inner_lift, inner_couple, inner_spread):
    devices, width, rank = parts.shape
    levels = devices.bit_length() - 1
    anywhere = pl.BlockSpec(memory_space=pl.ANY)
    inside = pl.BlockSpec(memory_space=pltpu.VMEM)
    return pl.pallas_call(
        functools.partial(tree_kernel, levels),
        out_shape=jax.ShapeDtypeStruct(parts.shape, jnp.bfloat16),
        in_specs=[inside, anywhere, anywhere, anywhere],
        out_specs=inside,
        scratch_shapes=[
            pltpu.VMEM(inner_lift.shape, jnp.bfloat16),
            pltpu.VMEM(inner_couple.shape, jnp.bfloat16),
            pltpu.VMEM(inner_spread.shape, jnp.bfloat16),
            pltpu.VMEM((inner_couple.shape[0], width, rank), jnp.float32),
            pltpu.SemaphoreType.DMA((3 * levels,)),
        ],
        compiler_params=pltpu.CompilerParams(vmem_limit_bytes=24 << 20),
        cost_estimate=pl.CostEstimate(
            flops=4 * 374 * 16 * 128 * 128, bytes_accessed=13 << 20, transcendentals=0
        ),
        name="tree",
    )(parts, inner_lift, inner_couple, inner_spread)


def local(
    basis_slab,
    live_counts,
    pole_order,
    leaf_diag,
    leaf_in,
    leaf_out,
    leaf_lift,
    leaf_couple,
    leaf_spread,
    inner_lift,
    inner_couple,
    inner_spread,
):
    devices = lax.axis_size("grp") * lax.axis_size("leaf")
    width, columns = basis_slab.shape
    rank = leaf_in.shape[1]
    block_rows = width // devices
    owned = columns // devices

    poles = exchange(basis_slab.reshape(devices, block_rows, columns)).reshape(width, columns)

    index = jnp.arange(width, dtype=jnp.int32)
    slot_pole = jnp.where(index < live_counts[0], pole_order[0], -1)
    select = (slot_pole[:, None] == index[None, :]).astype(jnp.bfloat16)
    is_live = jnp.any(slot_pole[:, None] == index[None, :], axis=0)
    generators = dot(select, jnp.concatenate([leaf_in, leaf_out], axis=1), TN).astype(jnp.bfloat16)
    in_poles, out_poles = generators[:, :rank], generators[:, rank:]
    rows = dot(select, leaf_diag, TN).astype(jnp.bfloat16)
    diag = dot(rows, select, (((1,), (0,)), ((), ())))
    dead_diag = (index[:, None] == index[None, :]) & ~is_live[:, None]
    diag = jnp.where(dead_diag, 1.0, diag).astype(jnp.bfloat16)

    skeleton = dot(poles, in_poles, TN)
    pair = split_rows(skeleton)
    lifted = times_transposed(pair, leaf_lift[0]).astype(jnp.bfloat16)
    coupled = times_transposed(pair, leaf_couple[0]).astype(jnp.bfloat16)
    leaves = lax.axis_size("leaf")
    cross = lax.ppermute(coupled, "leaf", [(i, i ^ 1) for i in range(leaves)])
    parts = exchange(lifted.reshape(devices, owned, rank))
    near = dot(diag, poles, (((1,), (0,)), ((), ())))
    above = exchange(tree(parts, inner_lift, inner_couple, inner_spread))
    incoming = dot(above.reshape(columns, rank), leaf_spread[0], NT) + cross.astype(jnp.float32)
    updated = near + dot(out_poles, incoming.astype(jnp.bfloat16), NT)
    merged = exchange(updated.astype(jnp.bfloat16).reshape(devices, block_rows, columns))
    return merged.reshape(width, columns)


def solution(mesh):
    placed = (
        P(BOTH, None),
        P(BOTH),
        P(BOTH, None),
        P(BOTH, None),
        P(BOTH, None),
        P(BOTH, None),
        P(BOTH, None, None),
        P(BOTH, None, None),
        P(BOTH, None, None),
        P(),
        P(),
        P(),
    )
    return jax.shard_map(
        local, mesh=mesh, in_specs=placed, out_specs=P(BOTH, None), check_vma=False
    )
```

```python
import functools

import jax
import jax.numpy as jnp
from jax import lax
from jax.experimental import pallas as pl
from jax.experimental.pallas import tpu as pltpu
from jax.sharding import PartitionSpec as P

BOTH = ("grp", "leaf")
NN = (((1,), (0,)), ((), ()))
NT = (((1,), (1,)), ((), ()))
TN = (((0,), (0,)), ((), ()))


def exchange(blocks):
    return lax.all_to_all(blocks, BOTH, split_axis=0, concat_axis=0, tiled=True)


def dot(a, b, dims):
    return lax.dot_general(a, b, dims, preferred_element_type=jnp.float32)


def split_rows(value):
    head = value.astype(jnp.bfloat16).astype(jnp.float32)
    return jnp.concatenate([head, value - head], axis=0).astype(jnp.bfloat16)


def kernel_options(mebibytes):
    return pltpu.CompilerParams(vmem_limit_bytes=mebibytes << 20)


def cost(flops, moved):
    return pl.CostEstimate(flops=flops, bytes_accessed=moved, transcendentals=0)


FAR = pl.BlockSpec(memory_space=pltpu.HBM)
INSIDE = pl.BlockSpec(memory_space=pltpu.VMEM)
TILE = 256


def fold_kernel(
    slot_ref, diag_hbm, both_ref, in_ref, out_ref, spread_ref,
    in_both_ref, out_poles_ref, out_spread_ref, folded_hbm,
    chosen, diag, folded, sems,
):
    width = diag.shape[0]
    load = pltpu.make_async_copy(diag_hbm, diag, sems.at[0])
    load.start()
    slots = slot_ref[...]
    for low in range(0, width, TILE):
        pole = lax.broadcasted_iota(jnp.int32, (TILE, width), 0) + low
        chosen[pl.ds(low, TILE)] = jnp.where(pole == slots, 1.0, 0.0).astype(jnp.bfloat16)
    in_poles = dot(chosen[...], in_ref[...], NN).astype(jnp.bfloat16)
    in_both_ref[...] = dot(both_ref[...], in_poles, NT).astype(jnp.bfloat16)
    out_poles = dot(chosen[...], out_ref[...], NN).astype(jnp.bfloat16)
    out_poles_ref[...] = out_poles
    out_spread_ref[...] = dot(out_poles, spread_ref[...], NN).astype(jnp.bfloat16)
    load.wait()
    stores = []
    for number, low in enumerate(range(0, width, TILE)):
        piece = pl.ds(low, TILE)
        rows = dot(chosen[piece], diag[...], NN).astype(jnp.bfloat16)
        value = dot(rows, chosen[...], NT)
        pole = lax.broadcasted_iota(jnp.int32, (TILE, width), 0) + low
        other = lax.broadcasted_iota(jnp.int32, (TILE, width), 1)
        live = jnp.sum(chosen[piece].astype(jnp.float32), axis=1, keepdims=True)
        value = jnp.where((pole == other) & (live < 0.5), 1.0, value)
        folded[piece] = value.astype(jnp.bfloat16)
        store = pltpu.make_async_copy(
            folded.at[piece], folded_hbm.at[piece], sems.at[1 + number]
        )
        store.start()
        stores.append(store)
    for store in stores:
        store.wait()


def fold(slot_pole, leaf_diag, both, leaf_in, leaf_out, spread):
    width = leaf_diag.shape[0]
    rank = leaf_in.shape[1]
    square = pltpu.VMEM((width, width), jnp.bfloat16)
    tall = jax.ShapeDtypeStruct((width, rank), jnp.bfloat16)
    return pl.pallas_call(
        fold_kernel,
        out_shape=(
            jax.ShapeDtypeStruct((2 * rank, width), jnp.bfloat16),
            tall,
            tall,
            pltpu.HBM((width, width), jnp.bfloat16),
        ),
        in_specs=[INSIDE, FAR, INSIDE, INSIDE, INSIDE, INSIDE],
        out_specs=(INSIDE, INSIDE, INSIDE, FAR),
        scratch_shapes=[square, square, square, pltpu.SemaphoreType.DMA((1 + width // TILE,))],
        compiler_params=kernel_options(32),
        cost_estimate=cost(5 * width**3, 6 << 20),
        name="fold",
    )(slot_pole, in_hbm(leaf_diag), both, leaf_in, leaf_out, spread)


def rise_kernel(rows_ref, poles_ref, lifted_ref, coupled_ref):
    rank = lifted_ref.shape[1]
    for low in range(0, poles_ref.shape[1], TILE):
        value = dot(rows_ref[...], poles_ref[:, pl.ds(low, TILE)], NN)
        value = value.T.astype(jnp.bfloat16)
        lifted_ref[pl.ds(low, TILE)] = value[:, :rank]
        coupled_ref[pl.ds(low, TILE)] = value[:, rank:]


def rise(rows, poles, rank):
    width, columns = poles.shape
    out = jax.ShapeDtypeStruct((columns, rank), jnp.bfloat16)
    return pl.pallas_call(
        rise_kernel,
        out_shape=(out, out),
        in_specs=[INSIDE, INSIDE],
        out_specs=(INSIDE, INSIDE),
        compiler_params=kernel_options(16),
        cost_estimate=cost(2 * rows.shape[0] * width * columns, 3 << 20),
        name="rise",
    )(rows, poles)


def in_hbm(array):
    return pltpu.with_memory_space_constraint(array, pltpu.HBM)


def tree_kernel(
    levels, parts_ref, lift_hbm, couple_hbm, spread_hbm, out_ref, lift, couple, spread, cross, sems
):
    inner = levels - 1
    count = 1 << inner
    rank = parts_ref.shape[2]
    copies = {}
    number = 0

    def fetch(first, source, target, offset, start, stop):
        nonlocal number
        piece = pl.ds(start - offset, stop - start)
        copy = pltpu.make_async_copy(source.at[piece], target.at[piece], sems.at[number])
        copy.start()
        copies.setdefault(first, []).append(copy)
        number += 1

    half, quarter, middle = count // 2, count // 4, count + count // 2
    for first, start, stop in (
        (count, count, middle),
        (middle, middle, 2 * count),
        (half, half, count),
        (quarter, 2, half),
    ):
        fetch(("up", first), lift_hbm, lift, 4, max(start, 4), stop)
        fetch(("up", first), couple_hbm, couple, 2, start, stop)
    for start, stop in ((4, half), (half, count), (count, 2 * count)):
        fetch(("down", start), spread_hbm, spread, 4, start, stop)

    def arrived(way, node):
        for copy in copies.get((way, node), ()):
            copy.wait()

    def apart(first, second):
        first, second = split_rows(first), split_rows(second)
        blank = jnp.zeros_like(first)
        return jnp.concatenate(
            [
                jnp.concatenate([first, blank], axis=1),
                jnp.concatenate([blank, second], axis=1),
            ],
            axis=0,
        )

    def beside(first, second):
        return jnp.concatenate([first, second], axis=1)

    width = parts_ref.shape[1]

    def joined(rows):
        return rows[:width] + rows[width:]

    skeletons = {
        count + n: parts_ref[2 * n].astype(jnp.float32) + parts_ref[2 * n + 1].astype(jnp.float32)
        for n in range(count)
    }
    for height in range(1, levels):
        nodes = 1 << (levels - height)
        for node in range(nodes, 2 * nodes, 2):
            arrived("up", node)
            pair = apart(skeletons[node], skeletons[node + 1])
            couples = beside(couple[node - 2], couple[node - 1])
            if height < inner:
                lifts = beside(lift[node - 4], lift[node - 3])
                both = dot(pair, jnp.concatenate([lifts, couples], axis=0), NT)
                up, across = both[:, :rank], both[:, rank:]
                skeletons[node // 2] = joined(up[: 2 * width] + up[2 * width :])
            else:
                across = dot(pair, couples, NT)
            cross[node - 1] = joined(across[: 2 * width])
            cross[node - 2] = joined(across[2 * width :])
    incoming = {2: cross[0], 3: cross[1]}
    for height in range(inner - 1, 0, -1):
        nodes = 1 << (levels - height)
        for node in range(nodes, 2 * nodes, 4):
            arrived("down", node)
            pair = apart(incoming[node // 2], incoming[node // 2 + 1])
            matrices = jnp.concatenate(
                [
                    beside(spread[node - 4], spread[node - 2]),
                    beside(spread[node - 3], spread[node - 1]),
                ],
                axis=0,
            )
            both = dot(pair, matrices, NT)
            for child in range(4):
                rows = both[2 * width * (child // 2) :][: 2 * width]
                value = joined(rows[:, rank * (child % 2) :][:, :rank])
                incoming[node + child] = value + cross[node + child - 2]
    for n in range(count):
        value = incoming[count + n].astype(out_ref.dtype)
        out_ref[2 * n] = value
        out_ref[2 * n + 1] = value


def tree(parts, inner_lift, inner_couple, inner_spread):
    devices, width, rank = parts.shape
    levels = devices.bit_length() - 1
    return pl.pallas_call(
        functools.partial(tree_kernel, levels),
        out_shape=jax.ShapeDtypeStruct(parts.shape, jnp.bfloat16),
        in_specs=[INSIDE, FAR, FAR, FAR],
        out_specs=INSIDE,
        scratch_shapes=[
            pltpu.VMEM(inner_lift.shape, jnp.bfloat16),
            pltpu.VMEM(inner_couple.shape, jnp.bfloat16),
            pltpu.VMEM(inner_spread.shape, jnp.bfloat16),
            pltpu.VMEM((inner_couple.shape[0], width, rank), jnp.float32),
            pltpu.SemaphoreType.DMA((11,)),
        ],
        compiler_params=kernel_options(20),
        cost_estimate=cost(4 * 374 * 16 * 128 * 128, 13 << 20),
        name="tree",
    )(parts, in_hbm(inner_lift), in_hbm(inner_couple), in_hbm(inner_spread))


def near_kernel(diag_hbm, poles_hbm, out_poles_ref, cross_ref, near_ref, diag, poles, sems):
    width = diag.shape[0]
    whole = pltpu.make_async_copy(poles_hbm, poles, sems.at[width // TILE])
    whole.start()
    loads = []
    for number, low in enumerate(range(0, width, TILE)):
        piece = pl.ds(low, TILE)
        load = pltpu.make_async_copy(diag_hbm.at[piece], diag.at[piece], sems.at[number])
        load.start()
        loads.append(load)
    whole.wait()
    for number, low in enumerate(range(0, width, TILE)):
        piece = pl.ds(low, TILE)
        loads[number].wait()
        value = dot(diag[piece], poles[...], NN)
        value += dot(out_poles_ref[piece], cross_ref[...], NT)
        near_ref[piece] = value.astype(near_ref.dtype)


def near_field(diag, poles, out_poles, cross):
    width, columns = poles.shape
    rank = out_poles.shape[1]
    return pl.pallas_call(
        near_kernel,
        out_shape=jax.ShapeDtypeStruct((width, columns), jnp.bfloat16),
        in_specs=[FAR, FAR, INSIDE, INSIDE],
        out_specs=INSIDE,
        scratch_shapes=[
            pltpu.VMEM(diag.shape, jnp.bfloat16),
            pltpu.VMEM(poles.shape, jnp.bfloat16),
            pltpu.SemaphoreType.DMA((1 + width // TILE,)),
        ],
        compiler_params=kernel_options(24),
        cost_estimate=cost(2 * width * (width + rank) * columns, 7 << 20),
        name="near",
    )(in_hbm(diag), in_hbm(poles), out_poles, cross)


def fall_kernel(near_ref, out_spread_ref, above_ref, out_ref):
    for low in range(0, near_ref.shape[0], TILE):
        piece = pl.ds(low, TILE)
        far = dot(out_spread_ref[piece], above_ref[...], NT)
        out_ref[piece] = (near_ref[piece].astype(jnp.float32) + far).astype(out_ref.dtype)


def fall(near, out_spread, above):
    width, columns = near.shape
    rank = above.shape[1]
    return pl.pallas_call(
        fall_kernel,
        out_shape=jax.ShapeDtypeStruct((width, columns), jnp.bfloat16),
        in_specs=[INSIDE, INSIDE, INSIDE],
        out_specs=INSIDE,
        compiler_params=kernel_options(16),
        cost_estimate=cost(2 * width * rank * columns, 5 << 20),
        name="fall",
    )(near, out_spread, above)


def local(
    basis_slab,
    live_counts,
    pole_order,
    leaf_diag,
    leaf_in,
    leaf_out,
    leaf_lift,
    leaf_couple,
    leaf_spread,
    inner_lift,
    inner_couple,
    inner_spread,
):
    leaves = lax.axis_size("leaf")
    devices = lax.axis_size("grp") * leaves
    width, columns = basis_slab.shape
    rank = leaf_in.shape[1]
    block_rows = width // devices
    owned = columns // devices

    poles = exchange(basis_slab.reshape(devices, block_rows, columns)).reshape(width, columns)

    slot = lax.broadcasted_iota(jnp.int32, (1, width), 1)
    slot_pole = jnp.where(slot < live_counts[0], pole_order, -1)
    both = jnp.concatenate([leaf_lift[0], leaf_couple[0]], axis=0)
    in_both, out_poles, out_spread, diag = fold(
        slot_pole, leaf_diag, both, leaf_in, leaf_out, leaf_spread[0]
    )
    lifted, coupled = rise(in_both, poles, rank)
    parts = exchange(lifted.reshape(devices, owned, rank))
    inside = tree(parts, inner_lift, inner_couple, inner_spread)
    inside, coupled = lax.optimization_barrier((inside, coupled))
    above = exchange(inside).reshape(columns, rank)
    cross = lax.ppermute(coupled, "leaf", [(i, i ^ 1) for i in range(leaves)])
    near = near_field(diag, poles, out_poles, cross)
    updated = fall(near, out_spread, above)
    merged = exchange(updated.reshape(devices, block_rows, columns))
    return merged.reshape(width, columns)


def solution(mesh):
    placed = (
        P(BOTH, None),
        P(BOTH),
        P(BOTH, None),
        P(BOTH, None),
        P(BOTH, None),
        P(BOTH, None),
        P(BOTH, None, None),
        P(BOTH, None, None),
        P(BOTH, None, None),
        P(),
        P(),
        P(),
    )
    return jax.shard_map(
        local, mesh=mesh, in_specs=placed, out_specs=P(BOTH, None), check_vma=False
    )
```

```python
import functools

import jax
import jax.numpy as jnp
from jax import lax
from jax.experimental import pallas as pl
from jax.experimental.pallas import tpu as pltpu
from jax.sharding import PartitionSpec as P

BOTH = ("grp", "leaf")
NN = (((1,), (0,)), ((), ()))
NT = (((1,), (1,)), ((), ()))
TN = (((0,), (0,)), ((), ()))


def exchange(blocks):
    return lax.all_to_all(blocks, BOTH, split_axis=0, concat_axis=0, tiled=True)


def dot(a, b, dims):
    return lax.dot_general(a, b, dims, preferred_element_type=jnp.float32)


def split_rows(value):
    head = value.astype(jnp.bfloat16).astype(jnp.float32)
    return jnp.concatenate([head, value - head], axis=0).astype(jnp.bfloat16)


def kernel_options(mebibytes):
    return pltpu.CompilerParams(vmem_limit_bytes=mebibytes << 20)


def cost(flops, moved):
    return pl.CostEstimate(flops=flops, bytes_accessed=moved, transcendentals=0)


COVER_FLOPS = 1 << 33
FAR = pl.BlockSpec(memory_space=pltpu.HBM)
INSIDE = pl.BlockSpec(memory_space=pltpu.VMEM)
TILE = 256


def fold_kernel(
    slot_ref, diag_hbm, both_ref, in_ref, out_ref, spread_ref,
    lift_hbm, couple_hbm, inner_spread_hbm,
    in_both_ref, out_poles_ref, out_spread_ref, folded_hbm, up_hbm, down_hbm, top_ref,
    chosen, diag, folded, lift, couple, spread, up, down, unit, sems,
):
    width = diag.shape[0]
    load = pltpu.make_async_copy(diag_hbm, diag, sems.at[0])
    load.start()
    inner_loads = [
        pltpu.make_async_copy(source, target, sems.at[1 + width // TILE + number])
        for number, (source, target) in enumerate(
            ((lift_hbm, lift), (couple_hbm, couple), (inner_spread_hbm, spread))
        )
    ]
    for copy in inner_loads:
        copy.start()
    slots = slot_ref[...]
    for low in range(0, width, TILE):
        pole = lax.broadcasted_iota(jnp.int32, (TILE, width), 0) + low
        chosen[pl.ds(low, TILE)] = jnp.where(pole == slots, 1.0, 0.0).astype(jnp.bfloat16)
    in_poles = dot(chosen[...], in_ref[...], NN).astype(jnp.bfloat16)
    in_both_ref[...] = dot(both_ref[...], in_poles, NT).astype(jnp.bfloat16)
    out_poles = dot(chosen[...], out_ref[...], NN).astype(jnp.bfloat16)
    out_poles_ref[...] = out_poles
    out_spread_ref[...] = dot(out_poles, spread_ref[...], NN).astype(jnp.bfloat16)
    load.wait()
    stores = []
    for number, low in enumerate(range(0, width, TILE)):
        piece = pl.ds(low, TILE)
        rows = dot(chosen[piece], diag[...], NN).astype(jnp.bfloat16)
        value = dot(rows, chosen[...], NT)
        pole = lax.broadcasted_iota(jnp.int32, (TILE, width), 0) + low
        other = lax.broadcasted_iota(jnp.int32, (TILE, width), 1)
        live = jnp.sum(chosen[piece].astype(jnp.float32), axis=1, keepdims=True)
        value = jnp.where((pole == other) & (live < 0.5), 1.0, value)
        folded[piece] = value.astype(jnp.bfloat16)
        store = pltpu.make_async_copy(
            folded.at[piece], folded_hbm.at[piece], sems.at[1 + number]
        )
        store.start()
        stores.append(store)
    side = unit.shape[0]
    row = lax.broadcasted_iota(jnp.int32, (side, side), 0)
    column = lax.broadcasted_iota(jnp.int32, (side, side), 1)
    unit[...] = jnp.where(row == column, 1.0, 0.0).astype(jnp.bfloat16)
    for copy in inner_loads:
        copy.wait()

    top_ref[...] = couple[:2]

    def square(first, second, third, fourth):
        top = jnp.concatenate([first, second], axis=1)
        return jnp.concatenate([top, jnp.concatenate([third, fourth], axis=1)], axis=0)

    def transposed(matrix):
        return dot(unit[...], matrix, NT).astype(jnp.bfloat16)

    def quad(number, carry):
        n = 4 * number
        for low in (0, 2):
            up[2 * number + low // 2] = transposed(
                square(
                    lift[n + low], lift[n + low + 1], couple[n + low + 2], couple[n + low + 3]
                )
            )
        down[number] = transposed(square(spread[n], spread[n + 2], spread[n + 1], spread[n + 3]))
        return carry

    lax.fori_loop(0, down.shape[0], quad, 0)
    for number, (source, target) in enumerate(((up, up_hbm), (down, down_hbm))):
        store = pltpu.make_async_copy(source, target, sems.at[4 + width // TILE + number])
        store.start()
        stores.append(store)
    for store in stores:
        store.wait()


def fold(
    slot_pole, leaf_diag, both, leaf_in, leaf_out, spread, inner_lift, inner_couple, inner_spread
):
    width = leaf_diag.shape[0]
    rank = leaf_in.shape[1]
    nodes = inner_lift.shape[0]
    up = (nodes // 2, 2 * rank, 2 * rank)
    down = (nodes // 4, 2 * rank, 2 * rank)
    square = pltpu.VMEM((width, width), jnp.bfloat16)
    tall = jax.ShapeDtypeStruct((width, rank), jnp.bfloat16)
    return pl.pallas_call(
        fold_kernel,
        out_shape=(
            jax.ShapeDtypeStruct((2 * rank, width), jnp.bfloat16),
            pltpu.HBM((width, rank), jnp.bfloat16),
            pltpu.HBM((width, rank), jnp.bfloat16),
            pltpu.HBM((width, width), jnp.bfloat16),
            pltpu.HBM(up, jnp.bfloat16),
            pltpu.HBM(down, jnp.bfloat16),
            jax.ShapeDtypeStruct((2, rank, rank), jnp.bfloat16),
        ),
        in_specs=[INSIDE, FAR, INSIDE, INSIDE, INSIDE, INSIDE, FAR, FAR, FAR],
        out_specs=(INSIDE, INSIDE, INSIDE, FAR, FAR, FAR, INSIDE),
        scratch_shapes=[
            square,
            square,
            square,
            pltpu.VMEM(inner_lift.shape, jnp.bfloat16),
            pltpu.VMEM(inner_couple.shape, jnp.bfloat16),
            pltpu.VMEM(inner_spread.shape, jnp.bfloat16),
            pltpu.VMEM(up, jnp.bfloat16),
            pltpu.VMEM(down, jnp.bfloat16),
            pltpu.VMEM((2 * rank, 2 * rank), jnp.bfloat16),
            pltpu.SemaphoreType.DMA((6 + width // TILE,)),
        ],
        compiler_params=kernel_options(48),
        cost_estimate=cost(8 * width**3, 30 << 20),
        name="fold",
    )(
        slot_pole,
        in_hbm(leaf_diag),
        both,
        leaf_in,
        leaf_out,
        spread,
        in_hbm(inner_lift),
        in_hbm(inner_couple),
        in_hbm(inner_spread),
    )


def rise_kernel(rows_ref, poles_ref, lifted_ref, coupled_ref):
    rank = lifted_ref.shape[1]
    for low in range(0, poles_ref.shape[1], TILE):
        value = dot(rows_ref[...], poles_ref[:, pl.ds(low, TILE)], NN)
        value = value.T.astype(jnp.bfloat16)
        lifted_ref[pl.ds(low, TILE)] = value[:, :rank]
        coupled_ref[pl.ds(low, TILE)] = value[:, rank:]


def rise(rows, poles, rank):
    width, columns = poles.shape
    out = jax.ShapeDtypeStruct((columns, rank), jnp.bfloat16)
    return pl.pallas_call(
        rise_kernel,
        out_shape=(out, out),
        in_specs=[INSIDE, INSIDE],
        out_specs=(INSIDE, INSIDE),
        compiler_params=kernel_options(16),
        cost_estimate=cost(COVER_FLOPS, 3 << 20),
        name="rise",
    )(rows, poles)


def in_hbm(array):
    return pltpu.with_memory_space_constraint(array, pltpu.HBM)


def tree_kernel(levels, parts_ref, up, down, top, out_ref, cross):
    inner = levels - 1
    count = 1 << inner
    rank = parts_ref.shape[2]

    def apart(first, second):
        first, second = split_rows(first), split_rows(second)
        blank = jnp.zeros_like(first)
        return jnp.concatenate(
            [
                jnp.concatenate([first, blank], axis=1),
                jnp.concatenate([blank, second], axis=1),
            ],
            axis=0,
        )

    def beside(first, second):
        return jnp.concatenate([first, second], axis=1)

    width = parts_ref.shape[1]

    def joined(rows):
        return rows[:width] + rows[width:]

    skeletons = {
        count + n: parts_ref[2 * n].astype(jnp.float32) + parts_ref[2 * n + 1].astype(jnp.float32)
        for n in range(count)
    }
    for height in range(1, levels):
        nodes = 1 << (levels - height)
        for node in range(nodes, 2 * nodes, 2):
            pair = apart(skeletons[node], skeletons[node + 1])
            if height < inner:
                both = dot(pair, up[node // 2 - 2], NN)
                lifted, across = both[:, :rank], both[:, rank:]
                skeletons[node // 2] = joined(lifted[: 2 * width] + lifted[2 * width :])
            else:
                across = dot(pair, beside(top[0], top[1]), NT)
            cross[node - 1] = joined(across[: 2 * width])
            cross[node - 2] = joined(across[2 * width :])
    incoming = {2: cross[0], 3: cross[1]}
    for height in range(inner - 1, 0, -1):
        nodes = 1 << (levels - height)
        for node in range(nodes, 2 * nodes, 4):
            pair = apart(incoming[node // 2], incoming[node // 2 + 1])
            both = dot(pair, down[node // 4 - 1], NN)
            for child in range(4):
                rows = both[2 * width * (child // 2) :][: 2 * width]
                value = joined(rows[:, rank * (child % 2) :][:, :rank])
                incoming[node + child] = value + cross[node + child - 2]
    for n in range(count):
        value = incoming[count + n].astype(out_ref.dtype)
        out_ref[2 * n] = value
        out_ref[2 * n + 1] = value


def tree(parts, up, down, top):
    devices, width, rank = parts.shape
    levels = devices.bit_length() - 1
    return pl.pallas_call(
        functools.partial(tree_kernel, levels),
        out_shape=jax.ShapeDtypeStruct(parts.shape, jnp.bfloat16),
        in_specs=[INSIDE] * 4,
        out_specs=INSIDE,
        scratch_shapes=[pltpu.VMEM((devices - 2, width, rank), jnp.float32)],
        compiler_params=kernel_options(4),
        cost_estimate=cost(4 * 374 * 16 * 128 * 128, 13 << 20),
        name="tree",
    )(parts, up, down, top)


def near_kernel(diag_hbm, poles_hbm, out_poles_ref, cross_ref, near_ref, diag, poles, sems):
    width = diag.shape[0]
    whole = pltpu.make_async_copy(poles_hbm, poles, sems.at[width // TILE])
    whole.start()
    loads = []
    for number, low in enumerate(range(0, width, TILE)):
        piece = pl.ds(low, TILE)
        load = pltpu.make_async_copy(diag_hbm.at[piece], diag.at[piece], sems.at[number])
        load.start()
        loads.append(load)
    whole.wait()
    for number, low in enumerate(range(0, width, TILE)):
        piece = pl.ds(low, TILE)
        loads[number].wait()
        value = dot(diag[piece], poles[...], NN)
        value += dot(out_poles_ref[piece], cross_ref[...], NT)
        near_ref[piece] = value.astype(near_ref.dtype)


def near_field(diag, poles, out_poles, cross):
    width, columns = poles.shape
    rank = out_poles.shape[1]
    return pl.pallas_call(
        near_kernel,
        out_shape=jax.ShapeDtypeStruct((width, columns), jnp.bfloat16),
        in_specs=[FAR, FAR, INSIDE, INSIDE],
        out_specs=INSIDE,
        scratch_shapes=[
            pltpu.VMEM(diag.shape, jnp.bfloat16),
            pltpu.VMEM(poles.shape, jnp.bfloat16),
            pltpu.SemaphoreType.DMA((1 + width // TILE,)),
        ],
        compiler_params=kernel_options(24),
        cost_estimate=cost(2 * width * (width + rank) * columns, 7 << 20),
        name="near",
    )(in_hbm(diag), in_hbm(poles), out_poles, cross)


def fall_kernel(near_ref, out_spread_ref, above_ref, out_ref):
    for low in range(0, near_ref.shape[0], TILE):
        piece = pl.ds(low, TILE)
        far = dot(out_spread_ref[piece], above_ref[...], NT)
        out_ref[piece] = (near_ref[piece].astype(jnp.float32) + far).astype(out_ref.dtype)


def fall(near, out_spread, above):
    width, columns = near.shape
    rank = above.shape[1]
    return pl.pallas_call(
        fall_kernel,
        out_shape=jax.ShapeDtypeStruct((width, columns), jnp.bfloat16),
        in_specs=[INSIDE, INSIDE, INSIDE],
        out_specs=INSIDE,
        compiler_params=kernel_options(16),
        cost_estimate=cost(2 * width * rank * columns, 5 << 20),
        name="fall",
    )(near, out_spread, above)


def local(
    basis_slab,
    live_counts,
    pole_order,
    leaf_diag,
    leaf_in,
    leaf_out,
    leaf_lift,
    leaf_couple,
    leaf_spread,
    inner_lift,
    inner_couple,
    inner_spread,
):
    leaves = lax.axis_size("leaf")
    devices = lax.axis_size("grp") * leaves
    width, columns = basis_slab.shape
    rank = leaf_in.shape[1]
    block_rows = width // devices
    owned = columns // devices

    poles = exchange(basis_slab.reshape(devices, block_rows, columns)).reshape(width, columns)

    slot = lax.broadcasted_iota(jnp.int32, (1, width), 1)
    slot_pole = jnp.where(slot < live_counts[0], pole_order, -1)
    both = jnp.concatenate([leaf_lift[0], leaf_couple[0]], axis=0)
    in_both, out_poles, out_spread, diag, up, down, top = fold(
        slot_pole,
        leaf_diag,
        both,
        leaf_in,
        leaf_out,
        leaf_spread[0],
        inner_lift,
        inner_couple,
        inner_spread,
    )
    lifted, coupled = rise(in_both, poles, rank)
    parts = exchange(lifted.reshape(devices, owned, rank))
    inside = tree(parts, up, down, top)
    inside, coupled = lax.optimization_barrier((inside, coupled))
    above = exchange(inside).reshape(columns, rank)
    cross = lax.ppermute(coupled, "leaf", [(i, i ^ 1) for i in range(leaves)])
    near = near_field(diag, poles, out_poles, cross)
    updated = fall(near, out_spread, above)
    merged = exchange(updated.reshape(devices, block_rows, columns))
    return merged.reshape(width, columns)


def solution(mesh):
    placed = (
        P(BOTH, None),
        P(BOTH),
        P(BOTH, None),
        P(BOTH, None),
        P(BOTH, None),
        P(BOTH, None),
        P(BOTH, None, None),
        P(BOTH, None, None),
        P(BOTH, None, None),
        P(),
        P(),
        P(),
    )
    return jax.shard_map(
        local, mesh=mesh, in_specs=placed, out_specs=P(BOTH, None), check_vma=False
    )
```

```python
import functools

import jax
import jax.numpy as jnp
from jax import lax
from jax.experimental import pallas as pl
from jax.experimental.pallas import tpu as pltpu
from jax.sharding import PartitionSpec as P

BOTH = ("grp", "leaf")
NN = (((1,), (0,)), ((), ()))
NT = (((1,), (1,)), ((), ()))
TN = (((0,), (0,)), ((), ()))


def exchange(blocks):
    return lax.all_to_all(blocks, BOTH, split_axis=0, concat_axis=0, tiled=True)


def dot(a, b, dims):
    return lax.dot_general(a, b, dims, preferred_element_type=jnp.float32)


def split_rows(value):
    head = value.astype(jnp.bfloat16).astype(jnp.float32)
    return jnp.concatenate([head, value - head], axis=0).astype(jnp.bfloat16)


def kernel_options(mebibytes):
    return pltpu.CompilerParams(vmem_limit_bytes=mebibytes << 20)


def cost(flops, moved):
    return pl.CostEstimate(flops=flops, bytes_accessed=moved, transcendentals=0)


COVER_FLOPS = 1 << 33
FAR = pl.BlockSpec(memory_space=pltpu.HBM)
INSIDE = pl.BlockSpec(memory_space=pltpu.VMEM)
TILE = 256


def fold_kernel(
    slot_ref, diag_hbm, both_ref, in_ref, out_ref, spread_ref,
    lift_hbm, couple_hbm, inner_spread_hbm,
    in_both_ref, out_poles_ref, out_spread_ref, folded_hbm, up_hbm, down_hbm, top_ref,
    chosen, diag, folded, lift, couple, spread, up, down, unit, sems,
):
    width = diag.shape[0]
    load = pltpu.make_async_copy(diag_hbm, diag, sems.at[0])
    load.start()
    inner_loads = [
        pltpu.make_async_copy(source, target, sems.at[1 + width // TILE + number])
        for number, (source, target) in enumerate(
            ((lift_hbm, lift), (couple_hbm, couple), (inner_spread_hbm, spread))
        )
    ]
    for copy in inner_loads:
        copy.start()
    slots = slot_ref[...]
    for low in range(0, width, TILE):
        pole = lax.broadcasted_iota(jnp.int32, (TILE, width), 0) + low
        chosen[pl.ds(low, TILE)] = jnp.where(pole == slots, 1.0, 0.0).astype(jnp.bfloat16)
    in_poles = dot(chosen[...], in_ref[...], NN).astype(jnp.bfloat16)
    in_both_ref[...] = dot(both_ref[...], in_poles, NT).astype(jnp.bfloat16)
    out_poles = dot(chosen[...], out_ref[...], NN).astype(jnp.bfloat16)
    out_poles_ref[...] = out_poles
    out_spread_ref[...] = dot(out_poles, spread_ref[...], NN).astype(jnp.bfloat16)
    load.wait()
    stores = []
    for number, low in enumerate(range(0, width, TILE)):
        piece = pl.ds(low, TILE)
        rows = dot(chosen[piece], diag[...], NN).astype(jnp.bfloat16)
        value = dot(rows, chosen[...], NT)
        pole = lax.broadcasted_iota(jnp.int32, (TILE, width), 0) + low
        other = lax.broadcasted_iota(jnp.int32, (TILE, width), 1)
        live = jnp.sum(chosen[piece].astype(jnp.float32), axis=1, keepdims=True)
        value = jnp.where((pole == other) & (live < 0.5), 1.0, value)
        folded[piece] = value.astype(jnp.bfloat16)
        store = pltpu.make_async_copy(
            folded.at[piece], folded_hbm.at[piece], sems.at[1 + number]
        )
        store.start()
        stores.append(store)
    side = unit.shape[0]
    row = lax.broadcasted_iota(jnp.int32, (side, side), 0)
    column = lax.broadcasted_iota(jnp.int32, (side, side), 1)
    unit[...] = jnp.where(row == column, 1.0, 0.0).astype(jnp.bfloat16)
    for copy in inner_loads:
        copy.wait()

    top_ref[...] = couple[:2]

    def square(first, second, third, fourth):
        top = jnp.concatenate([first, second], axis=1)
        return jnp.concatenate([top, jnp.concatenate([third, fourth], axis=1)], axis=0)

    def transposed(matrix):
        return dot(unit[...], matrix, NT).astype(jnp.bfloat16)

    def quad(number, carry):
        n = 4 * number
        for low in (0, 2):
            up[2 * number + low // 2] = transposed(
                square(
                    lift[n + low], lift[n + low + 1], couple[n + low + 2], couple[n + low + 3]
                )
            )
        down[number] = transposed(square(spread[n], spread[n + 2], spread[n + 1], spread[n + 3]))
        return carry

    lax.fori_loop(0, down.shape[0], quad, 0)
    for number, (source, target) in enumerate(((up, up_hbm), (down, down_hbm))):
        store = pltpu.make_async_copy(source, target, sems.at[4 + width // TILE + number])
        store.start()
        stores.append(store)
    for store in stores:
        store.wait()


def fold(
    slot_pole, leaf_diag, both, leaf_in, leaf_out, spread, inner_lift, inner_couple, inner_spread
):
    width = leaf_diag.shape[0]
    rank = leaf_in.shape[1]
    nodes = inner_lift.shape[0]
    up = (nodes // 2, 2 * rank, 2 * rank)
    down = (nodes // 4, 2 * rank, 2 * rank)
    square = pltpu.VMEM((width, width), jnp.bfloat16)
    tall = jax.ShapeDtypeStruct((width, rank), jnp.bfloat16)
    return pl.pallas_call(
        fold_kernel,
        out_shape=(
            jax.ShapeDtypeStruct((2 * rank, width), jnp.bfloat16),
            pltpu.HBM((width, rank), jnp.bfloat16),
            pltpu.HBM((width, rank), jnp.bfloat16),
            pltpu.HBM((width, width), jnp.bfloat16),
            pltpu.HBM(up, jnp.bfloat16),
            pltpu.HBM(down, jnp.bfloat16),
            jax.ShapeDtypeStruct((2, rank, rank), jnp.bfloat16),
        ),
        in_specs=[INSIDE, FAR, INSIDE, INSIDE, INSIDE, INSIDE, FAR, FAR, FAR],
        out_specs=(INSIDE, INSIDE, INSIDE, FAR, FAR, FAR, INSIDE),
        scratch_shapes=[
            square,
            square,
            square,
            pltpu.VMEM(inner_lift.shape, jnp.bfloat16),
            pltpu.VMEM(inner_couple.shape, jnp.bfloat16),
            pltpu.VMEM(inner_spread.shape, jnp.bfloat16),
            pltpu.VMEM(up, jnp.bfloat16),
            pltpu.VMEM(down, jnp.bfloat16),
            pltpu.VMEM((2 * rank, 2 * rank), jnp.bfloat16),
            pltpu.SemaphoreType.DMA((6 + width // TILE,)),
        ],
        compiler_params=kernel_options(48),
        cost_estimate=cost(8 * width**3, 30 << 20),
        name="fold",
    )(
        slot_pole,
        in_hbm(leaf_diag),
        both,
        leaf_in,
        leaf_out,
        spread,
        in_hbm(inner_lift),
        in_hbm(inner_couple),
        in_hbm(inner_spread),
    )


def rise_kernel(rows_ref, poles_ref, lifted_ref, coupled_ref):
    rank = lifted_ref.shape[1]
    for low in range(0, poles_ref.shape[1], TILE):
        value = dot(rows_ref[...], poles_ref[:, pl.ds(low, TILE)], NN)
        value = value.T.astype(jnp.bfloat16)
        lifted_ref[pl.ds(low, TILE)] = value[:, :rank]
        coupled_ref[pl.ds(low, TILE)] = value[:, rank:]


def rise(rows, poles, rank):
    width, columns = poles.shape
    out = jax.ShapeDtypeStruct((columns, rank), jnp.bfloat16)
    return pl.pallas_call(
        rise_kernel,
        out_shape=(out, out),
        in_specs=[INSIDE, INSIDE],
        out_specs=(INSIDE, INSIDE),
        compiler_params=kernel_options(16),
        cost_estimate=cost(COVER_FLOPS, 3 << 20),
        name="rise",
    )(rows, poles)


def in_hbm(array):
    return pltpu.with_memory_space_constraint(array, pltpu.HBM)


def tree_kernel(levels, parts_ref, up, down, top, out_ref, cross):
    inner = levels - 1
    count = 1 << inner
    rank = parts_ref.shape[2]

    def apart(first, second):
        first, second = split_rows(first), split_rows(second)
        blank = jnp.zeros_like(first)
        return jnp.concatenate(
            [
                jnp.concatenate([first, blank], axis=1),
                jnp.concatenate([blank, second], axis=1),
            ],
            axis=0,
        )

    def beside(first, second):
        return jnp.concatenate([first, second], axis=1)

    width = parts_ref.shape[1]

    def joined(rows):
        return rows[:width] + rows[width:]

    skeletons = {
        count + n: parts_ref[2 * n].astype(jnp.float32) + parts_ref[2 * n + 1].astype(jnp.float32)
        for n in range(count)
    }
    for height in range(1, levels):
        nodes = 1 << (levels - height)
        for node in range(nodes, 2 * nodes, 2):
            pair = apart(skeletons[node], skeletons[node + 1])
            if height < inner:
                both = dot(pair, up[node // 2 - 2], NN)
                lifted, across = both[:, :rank], both[:, rank:]
                skeletons[node // 2] = joined(lifted[: 2 * width] + lifted[2 * width :])
            else:
                across = dot(pair, beside(top[0], top[1]), NT)
            cross[node - 1] = joined(across[: 2 * width])
            cross[node - 2] = joined(across[2 * width :])
    incoming = {2: cross[0], 3: cross[1]}
    for height in range(inner - 1, 0, -1):
        nodes = 1 << (levels - height)
        for node in range(nodes, 2 * nodes, 4):
            pair = apart(incoming[node // 2], incoming[node // 2 + 1])
            both = dot(pair, down[node // 4 - 1], NN)
            for child in range(4):
                rows = both[2 * width * (child // 2) :][: 2 * width]
                value = joined(rows[:, rank * (child % 2) :][:, :rank])
                incoming[node + child] = value + cross[node + child - 2]
    for n in range(count):
        value = incoming[count + n].astype(out_ref.dtype)
        out_ref[2 * n] = value
        out_ref[2 * n + 1] = value


def tree(parts, up, down, top):
    devices, width, rank = parts.shape
    levels = devices.bit_length() - 1
    return pl.pallas_call(
        functools.partial(tree_kernel, levels),
        out_shape=jax.ShapeDtypeStruct(parts.shape, jnp.bfloat16),
        in_specs=[INSIDE] * 4,
        out_specs=INSIDE,
        scratch_shapes=[pltpu.VMEM((devices - 2, width, rank), jnp.float32)],
        compiler_params=kernel_options(4),
        cost_estimate=cost(4 * 374 * 16 * 128 * 128, 13 << 20),
        name="tree",
    )(parts, up, down, top)


def near_kernel(diag_hbm, poles_ref, out_poles_ref, cross_ref, near_ref, diag, sem):
    load = pltpu.make_async_copy(diag_hbm, diag, sem)
    load.start()
    load.wait()
    for low in range(0, poles_ref.shape[1], TILE):
        piece = pl.ds(low, TILE)
        value = dot(diag[...], poles_ref[:, piece], NN)
        value += dot(out_poles_ref[...], cross_ref[piece], NT)
        near_ref[:, piece] = value.astype(near_ref.dtype)


def near_field(diag, poles, out_poles, cross):
    width, columns = poles.shape
    rank = out_poles.shape[1]
    return pl.pallas_call(
        near_kernel,
        out_shape=jax.ShapeDtypeStruct((width, columns), jnp.bfloat16),
        in_specs=[FAR, INSIDE, INSIDE, INSIDE],
        out_specs=INSIDE,
        input_output_aliases={1: 0},
        scratch_shapes=[pltpu.VMEM(diag.shape, jnp.bfloat16), pltpu.SemaphoreType.DMA],
        compiler_params=kernel_options(24),
        cost_estimate=cost(2 * width * (width + rank) * columns, 7 << 20),
        name="near",
    )(in_hbm(diag), poles, out_poles, cross)


def fall_kernel(near_ref, out_spread_ref, above_ref, out_ref):
    for low in range(0, near_ref.shape[0], TILE):
        piece = pl.ds(low, TILE)
        far = dot(out_spread_ref[piece], above_ref[...], NT)
        out_ref[piece] = (near_ref[piece].astype(jnp.float32) + far).astype(out_ref.dtype)


def fall(near, out_spread, above):
    width, columns = near.shape
    rank = above.shape[1]
    return pl.pallas_call(
        fall_kernel,
        out_shape=jax.ShapeDtypeStruct((width, columns), jnp.bfloat16),
        in_specs=[INSIDE, INSIDE, INSIDE],
        out_specs=INSIDE,
        compiler_params=kernel_options(16),
        cost_estimate=cost(2 * width * rank * columns, 5 << 20),
        name="fall",
    )(near, out_spread, above)


def local(
    basis_slab,
    live_counts,
    pole_order,
    leaf_diag,
    leaf_in,
    leaf_out,
    leaf_lift,
    leaf_couple,
    leaf_spread,
    inner_lift,
    inner_couple,
    inner_spread,
):
    leaves = lax.axis_size("leaf")
    devices = lax.axis_size("grp") * leaves
    width, columns = basis_slab.shape
    rank = leaf_in.shape[1]
    block_rows = width // devices
    owned = columns // devices

    poles = exchange(basis_slab.reshape(devices, block_rows, columns)).reshape(width, columns)

    slot = lax.broadcasted_iota(jnp.int32, (1, width), 1)
    slot_pole = jnp.where(slot < live_counts[0], pole_order, -1)
    both = jnp.concatenate([leaf_lift[0], leaf_couple[0]], axis=0)
    in_both, out_poles, out_spread, diag, up, down, top = fold(
        slot_pole,
        leaf_diag,
        both,
        leaf_in,
        leaf_out,
        leaf_spread[0],
        inner_lift,
        inner_couple,
        inner_spread,
    )
    lifted, coupled = rise(in_both, poles, rank)
    parts = exchange(lifted.reshape(devices, owned, rank))
    inside = tree(parts, up, down, top)
    inside, coupled = lax.optimization_barrier((inside, coupled))
    above = exchange(inside).reshape(columns, rank)
    cross = lax.ppermute(coupled, "leaf", [(i, i ^ 1) for i in range(leaves)])
    near = near_field(diag, poles, out_poles, cross)
    updated = fall(near, out_spread, above)
    merged = exchange(updated.reshape(devices, block_rows, columns))
    return merged.reshape(width, columns)


def solution(mesh):
    placed = (
        P(BOTH, None),
        P(BOTH),
        P(BOTH, None),
        P(BOTH, None),
        P(BOTH, None),
        P(BOTH, None),
        P(BOTH, None, None),
        P(BOTH, None, None),
        P(BOTH, None, None),
        P(),
        P(),
        P(),
    )
    return jax.shard_map(
        local, mesh=mesh, in_specs=placed, out_specs=P(BOTH, None), check_vma=False
    )
```

```python
import functools

import jax
import jax.numpy as jnp
from jax import lax
from jax.experimental import pallas as pl
from jax.experimental.pallas import tpu as pltpu
from jax.sharding import PartitionSpec as P

BOTH = ("grp", "leaf")
NN = (((1,), (0,)), ((), ()))
NT = (((1,), (1,)), ((), ()))
TN = (((0,), (0,)), ((), ()))


def exchange(blocks):
    return lax.all_to_all(blocks, BOTH, split_axis=0, concat_axis=0, tiled=True)


def dot(a, b, dims):
    return lax.dot_general(a, b, dims, preferred_element_type=jnp.float32)


def split_rows(value):
    head = value.astype(jnp.bfloat16).astype(jnp.float32)
    return jnp.concatenate([head, value - head], axis=0).astype(jnp.bfloat16)


def kernel_options(mebibytes):
    return pltpu.CompilerParams(vmem_limit_bytes=mebibytes << 20)


def cost(flops, moved):
    return pl.CostEstimate(flops=flops, bytes_accessed=moved, transcendentals=0)


COVER_FLOPS = 1 << 33
FAR = pl.BlockSpec(memory_space=pltpu.HBM)
INSIDE = pl.BlockSpec(memory_space=pltpu.VMEM)
TILE = 256


def fold_kernel(
    slot_ref, diag_hbm, both_ref, in_ref, out_ref, spread_ref,
    lift_hbm, couple_hbm, inner_spread_hbm,
    in_both_ref, out_poles_ref, out_spread_ref, folded_hbm, up_hbm, down_hbm, top_ref,
    chosen, diag, folded, lift, couple, spread, up, down, unit, sems,
):
    width = diag.shape[0]
    load = pltpu.make_async_copy(diag_hbm, diag, sems.at[0])
    load.start()
    inner_loads = [
        pltpu.make_async_copy(source, target, sems.at[1 + width // TILE + number])
        for number, (source, target) in enumerate(
            ((lift_hbm, lift), (couple_hbm, couple), (inner_spread_hbm, spread))
        )
    ]
    for copy in inner_loads:
        copy.start()
    slots = slot_ref[...]
    for low in range(0, width, TILE):
        pole = lax.broadcasted_iota(jnp.int32, (TILE, width), 0) + low
        chosen[pl.ds(low, TILE)] = jnp.where(pole == slots, 1.0, 0.0).astype(jnp.bfloat16)
    in_poles = dot(chosen[...], in_ref[...], NN).astype(jnp.bfloat16)
    in_both_ref[...] = dot(both_ref[...], in_poles, NT).astype(jnp.bfloat16)
    out_poles = dot(chosen[...], out_ref[...], NN).astype(jnp.bfloat16)
    out_poles_ref[...] = out_poles
    out_spread_ref[...] = dot(out_poles, spread_ref[...], NN).astype(jnp.bfloat16)
    load.wait()
    stores = []
    for number, low in enumerate(range(0, width, TILE)):
        piece = pl.ds(low, TILE)
        rows = dot(chosen[piece], diag[...], NN).astype(jnp.bfloat16)
        value = dot(rows, chosen[...], NT)
        pole = lax.broadcasted_iota(jnp.int32, (TILE, width), 0) + low
        other = lax.broadcasted_iota(jnp.int32, (TILE, width), 1)
        live = jnp.sum(chosen[piece].astype(jnp.float32), axis=1, keepdims=True)
        value = jnp.where((pole == other) & (live < 0.5), 1.0, value)
        folded[piece] = value.astype(jnp.bfloat16)
        store = pltpu.make_async_copy(
            folded.at[piece], folded_hbm.at[piece], sems.at[1 + number]
        )
        store.start()
        stores.append(store)
    side = unit.shape[0]
    row = lax.broadcasted_iota(jnp.int32, (side, side), 0)
    column = lax.broadcasted_iota(jnp.int32, (side, side), 1)
    unit[...] = jnp.where(row == column, 1.0, 0.0).astype(jnp.bfloat16)
    for copy in inner_loads:
        copy.wait()

    top_ref[...] = couple[:2]

    def square(first, second, third, fourth):
        top = jnp.concatenate([first, second], axis=1)
        return jnp.concatenate([top, jnp.concatenate([third, fourth], axis=1)], axis=0)

    def transposed(matrix):
        return dot(unit[...], matrix, NT).astype(jnp.bfloat16)

    def quad(number):
        n = 4 * number
        for low in (0, 2):
            up[2 * number + low // 2] = transposed(
                square(
                    lift[n + low], lift[n + low + 1], couple[n + low + 2], couple[n + low + 3]
                )
            )
        down[number] = transposed(square(spread[n], spread[n + 2], spread[n + 1], spread[n + 3]))

    def several(step, carry):
        for number in range(4):
            quad(4 * step + number)
        return carry

    quads = down.shape[0]
    lax.fori_loop(0, quads // 4, several, 0)
    for number in range(quads // 4 * 4, quads):
        quad(number)
    for number, (source, target) in enumerate(((up, up_hbm), (down, down_hbm))):
        store = pltpu.make_async_copy(source, target, sems.at[4 + width // TILE + number])
        store.start()
        stores.append(store)
    for store in stores:
        store.wait()


def fold(
    slot_pole, leaf_diag, both, leaf_in, leaf_out, spread, inner_lift, inner_couple, inner_spread
):
    width = leaf_diag.shape[0]
    rank = leaf_in.shape[1]
    nodes = inner_lift.shape[0]
    up = (nodes // 2, 2 * rank, 2 * rank)
    down = (nodes // 4, 2 * rank, 2 * rank)
    square = pltpu.VMEM((width, width), jnp.bfloat16)
    tall = jax.ShapeDtypeStruct((width, rank), jnp.bfloat16)
    return pl.pallas_call(
        fold_kernel,
        out_shape=(
            jax.ShapeDtypeStruct((2 * rank, width), jnp.bfloat16),
            pltpu.HBM((width, rank), jnp.bfloat16),
            pltpu.HBM((width, rank), jnp.bfloat16),
            pltpu.HBM((width, width), jnp.bfloat16),
            pltpu.HBM(up, jnp.bfloat16),
            pltpu.HBM(down, jnp.bfloat16),
            jax.ShapeDtypeStruct((2, rank, rank), jnp.bfloat16),
        ),
        in_specs=[INSIDE, FAR, INSIDE, INSIDE, INSIDE, INSIDE, FAR, FAR, FAR],
        out_specs=(INSIDE, INSIDE, INSIDE, FAR, FAR, FAR, INSIDE),
        scratch_shapes=[
            square,
            square,
            square,
            pltpu.VMEM(inner_lift.shape, jnp.bfloat16),
            pltpu.VMEM(inner_couple.shape, jnp.bfloat16),
            pltpu.VMEM(inner_spread.shape, jnp.bfloat16),
            pltpu.VMEM(up, jnp.bfloat16),
            pltpu.VMEM(down, jnp.bfloat16),
            pltpu.VMEM((2 * rank, 2 * rank), jnp.bfloat16),
            pltpu.SemaphoreType.DMA((6 + width // TILE,)),
        ],
        compiler_params=kernel_options(48),
        cost_estimate=cost(8 * width**3, 30 << 20),
        name="fold",
    )(
        slot_pole,
        in_hbm(leaf_diag),
        both,
        leaf_in,
        leaf_out,
        spread,
        in_hbm(inner_lift),
        in_hbm(inner_couple),
        in_hbm(inner_spread),
    )


def rise_kernel(rows_ref, poles_ref, lifted_ref, coupled_ref):
    rank = lifted_ref.shape[1]
    for low in range(0, poles_ref.shape[1], TILE):
        value = dot(rows_ref[...], poles_ref[:, pl.ds(low, TILE)], NN)
        value = value.T.astype(jnp.bfloat16)
        lifted_ref[pl.ds(low, TILE)] = value[:, :rank]
        coupled_ref[pl.ds(low, TILE)] = value[:, rank:]


def rise(rows, poles, rank):
    width, columns = poles.shape
    out = jax.ShapeDtypeStruct((columns, rank), jnp.bfloat16)
    return pl.pallas_call(
        rise_kernel,
        out_shape=(out, out),
        in_specs=[INSIDE, INSIDE],
        out_specs=(INSIDE, INSIDE),
        compiler_params=kernel_options(16),
        cost_estimate=cost(COVER_FLOPS, 3 << 20),
        name="rise",
    )(rows, poles)


def in_hbm(array):
    return pltpu.with_memory_space_constraint(array, pltpu.HBM)


def tree_kernel(levels, parts_ref, up, down, top, out_ref, cross):
    inner = levels - 1
    count = 1 << inner
    rank = parts_ref.shape[2]

    def apart(first, second):
        first, second = split_rows(first), split_rows(second)
        blank = jnp.zeros_like(first)
        return jnp.concatenate(
            [
                jnp.concatenate([first, blank], axis=1),
                jnp.concatenate([blank, second], axis=1),
            ],
            axis=0,
        )

    def beside(first, second):
        return jnp.concatenate([first, second], axis=1)

    width = parts_ref.shape[1]

    def joined(rows):
        return rows[:width] + rows[width:]

    skeletons = {
        count + n: parts_ref[2 * n].astype(jnp.float32) + parts_ref[2 * n + 1].astype(jnp.float32)
        for n in range(count)
    }
    for height in range(1, levels):
        nodes = 1 << (levels - height)
        for node in range(nodes, 2 * nodes, 2):
            pair = apart(skeletons[node], skeletons[node + 1])
            if height < inner:
                both = dot(pair, up[node // 2 - 2], NN)
                lifted, across = both[:, :rank], both[:, rank:]
                skeletons[node // 2] = joined(lifted[: 2 * width] + lifted[2 * width :])
            else:
                across = dot(pair, beside(top[0], top[1]), NT)
            cross[node - 1] = joined(across[: 2 * width])
            cross[node - 2] = joined(across[2 * width :])
    incoming = {2: cross[0], 3: cross[1]}
    for height in range(inner - 1, 0, -1):
        nodes = 1 << (levels - height)
        for node in range(nodes, 2 * nodes, 4):
            pair = apart(incoming[node // 2], incoming[node // 2 + 1])
            both = dot(pair, down[node // 4 - 1], NN)
            for child in range(4):
                rows = both[2 * width * (child // 2) :][: 2 * width]
                value = joined(rows[:, rank * (child % 2) :][:, :rank])
                incoming[node + child] = value + cross[node + child - 2]
    for n in range(count):
        value = incoming[count + n].astype(out_ref.dtype)
        out_ref[2 * n] = value
        out_ref[2 * n + 1] = value


def tree(parts, up, down, top):
    devices, width, rank = parts.shape
    levels = devices.bit_length() - 1
    return pl.pallas_call(
        functools.partial(tree_kernel, levels),
        out_shape=jax.ShapeDtypeStruct(parts.shape, jnp.bfloat16),
        in_specs=[INSIDE] * 4,
        out_specs=INSIDE,
        scratch_shapes=[pltpu.VMEM((devices - 2, width, rank), jnp.float32)],
        compiler_params=kernel_options(4),
        cost_estimate=cost(4 * 374 * 16 * 128 * 128, 13 << 20),
        name="tree",
    )(parts, up, down, top)


def near_kernel(diag_hbm, poles_ref, out_poles_ref, cross_ref, near_ref, diag, sem):
    load = pltpu.make_async_copy(diag_hbm, diag, sem)
    load.start()
    load.wait()
    for low in range(0, poles_ref.shape[1], TILE):
        piece = pl.ds(low, TILE)
        value = dot(diag[...], poles_ref[:, piece], NN)
        value += dot(out_poles_ref[...], cross_ref[piece], NT)
        near_ref[:, piece] = value.astype(near_ref.dtype)


def near_field(diag, poles, out_poles, cross):
    width, columns = poles.shape
    rank = out_poles.shape[1]
    return pl.pallas_call(
        near_kernel,
        out_shape=jax.ShapeDtypeStruct((width, columns), jnp.bfloat16),
        in_specs=[FAR, INSIDE, INSIDE, INSIDE],
        out_specs=INSIDE,
        input_output_aliases={1: 0},
        scratch_shapes=[pltpu.VMEM(diag.shape, jnp.bfloat16), pltpu.SemaphoreType.DMA],
        compiler_params=kernel_options(24),
        cost_estimate=cost(2 * width * (width + rank) * columns, 7 << 20),
        name="near",
    )(in_hbm(diag), poles, out_poles, cross)


def fall_kernel(near_ref, out_spread_ref, above_ref, out_ref):
    for low in range(0, near_ref.shape[0], TILE):
        piece = pl.ds(low, TILE)
        far = dot(out_spread_ref[piece], above_ref[...], NT)
        out_ref[piece] = (near_ref[piece].astype(jnp.float32) + far).astype(out_ref.dtype)


def fall(near, out_spread, above):
    width, columns = near.shape
    rank = above.shape[1]
    return pl.pallas_call(
        fall_kernel,
        out_shape=jax.ShapeDtypeStruct((width, columns), jnp.bfloat16),
        in_specs=[INSIDE, INSIDE, INSIDE],
        out_specs=INSIDE,
        compiler_params=kernel_options(16),
        cost_estimate=cost(2 * width * rank * columns, 5 << 20),
        name="fall",
    )(near, out_spread, above)


def local(
    basis_slab,
    live_counts,
    pole_order,
    leaf_diag,
    leaf_in,
    leaf_out,
    leaf_lift,
    leaf_couple,
    leaf_spread,
    inner_lift,
    inner_couple,
    inner_spread,
):
    leaves = lax.axis_size("leaf")
    devices = lax.axis_size("grp") * leaves
    width, columns = basis_slab.shape
    rank = leaf_in.shape[1]
    block_rows = width // devices
    owned = columns // devices

    poles = exchange(basis_slab.reshape(devices, block_rows, columns)).reshape(width, columns)

    slot = lax.broadcasted_iota(jnp.int32, (1, width), 1)
    slot_pole = jnp.where(slot < live_counts[0], pole_order, -1)
    both = jnp.concatenate([leaf_lift[0], leaf_couple[0]], axis=0)
    in_both, out_poles, out_spread, diag, up, down, top = fold(
        slot_pole,
        leaf_diag,
        both,
        leaf_in,
        leaf_out,
        leaf_spread[0],
        inner_lift,
        inner_couple,
        inner_spread,
    )
    lifted, coupled = rise(in_both, poles, rank)
    parts = exchange(lifted.reshape(devices, owned, rank))
    inside = tree(parts, up, down, top)
    inside, coupled = lax.optimization_barrier((inside, coupled))
    above = exchange(inside).reshape(columns, rank)
    cross = lax.ppermute(coupled, "leaf", [(i, i ^ 1) for i in range(leaves)])
    near = near_field(diag, poles, out_poles, cross)
    updated = fall(near, out_spread, above)
    merged = exchange(updated.reshape(devices, block_rows, columns))
    return merged.reshape(width, columns)


def solution(mesh):
    placed = (
        P(BOTH, None),
        P(BOTH),
        P(BOTH, None),
        P(BOTH, None),
        P(BOTH, None),
        P(BOTH, None),
        P(BOTH, None, None),
        P(BOTH, None, None),
        P(BOTH, None, None),
        P(),
        P(),
        P(),
    )
    return jax.shard_map(
        local, mesh=mesh, in_specs=placed, out_specs=P(BOTH, None), check_vma=False
    )
```
